32 devices in a mesh: clip: 8 (over z, x), frame: 4 (over y, core).
Axes of the slice: x: 2, y: 2, z: 4, core: 2. Of those that a mesh axis runs over, the one named last changes fastest.
Arguments:
- patches: bfloat16 [16, 4, 256, 768], P('clip', 'frame'), may hold values from -6 to 6
- mask_ids: int32 [16, 4, 256], P('clip', 'frame'), may hold values 0 or 1
- action_ids: int32 [16, 4], P('clip', 'frame'), may hold values from 0 to 255
- action_table: bfloat16 [256, 768], replicated, may hold values from -6 to 6
- action_proj: bfloat16 [768, 768], replicated, may hold values from -0.21875 to 0.21875
- mask_embed: float32 [768], replicated, may hold values from -6 to 6
- norm_gain: float32 [2, 2, 768], replicated, may hold values from 0.5 to 1.5
- norm_bias: float32 [2, 2, 768], replicated, may hold values from -3 to 3
- w_qkv: bfloat16 [2, 768, 2304], replicated, may hold values from -0.21875 to 0.21875
- qv_bias: float32 [2, 2, 768], replicated, may hold values from -3 to 3
- w_out: bfloat16 [2, 768, 768], replicated, may hold values from -0.875 to 0.875
- out_bias: float32 [2, 768], replicated, may hold values from -3 to 3
- w_fc1: bfloat16 [2, 768, 3072], replicated, may hold values from -0.21875 to 0.21875
- fc1_bias: float32 [2, 3072], replicated, may hold values from -3 to 3
- w_fc2: bfloat16 [2, 3072, 768], replicated, may hold values from -0.109375 to 0.109375
- fc2_bias: float32 [2, 768], replicated, may hold values from -3 to 3
- cotangent: bfloat16 [16, 4, 256, 768], P('clip', 'frame'), may hold values from -6 to 6
Outputs:
- output: bfloat16 [16, 4, 256, 768], P('clip', 'frame')
- patches_grad: bfloat16 [16, 4, 256, 768], P('clip', 'frame')
- action_table_grad: float32 [256, 768], P('clip', 'frame')
- action_proj_grad: float32 [768, 768], P('clip', 'frame')
- mask_embed_grad: float32 [768], replicated
- norm_gain_grad: float32 [2, 2, 768], replicated
- norm_bias_grad: float32 [2, 2, 768], replicated
- w_qkv_grad: float32 [2, 768, 2304], P(None, 'clip', 'frame')
- qv_bias_grad: float32 [2, 2, 768], replicated
- w_out_grad: float32 [2, 768, 768], P(None, 'clip', 'frame')
- out_bias_grad: float32 [2, 768], replicated
- w_fc1_grad: float32 [2, 768, 3072], P(None, 'clip', 'frame')
- fc1_bias_grad: float32 [2, 3072], replicated
- w_fc2_grad: float32 [2, 3072, 768], P(None, 'clip', 'frame')
- fc2_bias_grad: float32 [2, 768], replicated
The draws below stay inside these ranges and needn't reach their ends.
All inputs are finite; a program needn't handle non-finite values. No bound on the sum of `mask_ids` on one device may be relied on, other than what follows from the above.
Results may differ from the reference program's by a relative error of at most 0.018.
Values may be sent and summed in bfloat16 or wider, within the bound.
A program may use at most 192 MiB of HBM per device.

```python
import jax
import jax.numpy as jnp
from jax import lax

D = 768
HEADS = 12
FF = 3072
GRID = 16
TUBE_W = 4
NACT = 256
CLIPS = 16
FRAMES = 4
FRAME_TOK = 256


def touch_ends(values, rng, least, largest):
    spot = [jax.random.randint(jax.random.fold_in(rng, axis), (), 0, length) for axis, length in enumerate(values.shape)]
    longest = values.shape.index(max(values.shape))
    neighbour = spot[:longest] + [(spot[longest] + 1) % values.shape[longest]] + spot[longest + 1:]
    return values.at[tuple(spot)].set(least).at[tuple(neighbour)].set(largest)


def level_of(rng, extent, shards, smallest, top_value):
    def one(position, blocks):
        heights = jax.random.uniform(jax.random.fold_in(jax.random.fold_in(rng, 6), position), (blocks,), jnp.float32, smallest / len(shards), top_value / len(shards))
        return jnp.repeat(jnp.exp(heights), extent[position] // blocks).reshape((-1,) + (1,) * (len(extent) - position - 1))

    level = one(*shards[0])
    for cut in shards[1:]:
        level = level * one(*cut)
    return level


def gaussian(stream_key, dims, scale, most, pieces=(), held_as=jnp.bfloat16):
    loudness = level_of(stream_key, dims, pieces, -0.22, 0.18) if pieces else 1.0
    values = jax.random.normal(stream_key, dims, jnp.float32) * scale * loudness
    return jnp.minimum(jnp.maximum(values, -most), most).astype(held_as)


def setup_inputs(seed: int = 0) -> dict:
    keys = jax.random.split(jax.random.key(seed), 18)
    patches = gaussian(keys[0], (CLIPS, FRAMES, FRAME_TOK, D), 1.0, 6.0, ((0, 8), (1, 4)))
    mask_ids = touch_ends((jax.random.randint(keys[1], (CLIPS, FRAMES, FRAME_TOK), 0, 2) < 1).astype(jnp.int32), jax.random.fold_in(keys[1], 1), 0, 1)
    action_ids = touch_ends(jax.random.randint(keys[2], (CLIPS, FRAMES), 0, NACT), jax.random.fold_in(keys[2], 1), 0, NACT - 1).astype(jnp.int32)
    action_table = gaussian(keys[3], (NACT, D), 1.0, 6.0)
    action_proj = gaussian(keys[4], (D, D), D ** -0.5, 0.21875)
    mask_embed = gaussian(keys[5], (D,), 1.0, 6.0, (), jnp.float32)
    norm_gain = jnp.clip(1.0 + 0.1 * jax.random.normal(keys[6], (2, 2, D), jnp.float32), 0.5, 1.5)
    norm_bias = gaussian(keys[7], (2, 2, D), 0.5, 3.0, (), jnp.float32)
    w_qkv = gaussian(keys[8], (2, D, 3 * D), D ** -0.5, 0.21875)
    qv_bias = gaussian(keys[9], (2, 2, D), 0.5, 3.0, (), jnp.float32)
    w_out = gaussian(keys[10], (2, D, D), (D // 16) ** -0.5, 0.875)
    out_bias = gaussian(keys[11], (2, D), 0.5, 3.0, (), jnp.float32)
    w_fc1 = gaussian(keys[12], (2, D, FF), D ** -0.5, 0.21875)
    fc1_bias = gaussian(keys[13], (2, FF), 0.5, 3.0, (), jnp.float32)
    w_fc2 = gaussian(keys[14], (2, FF, D), FF ** -0.5, 0.109375)
    fc2_bias = gaussian(keys[15], (2, D), 0.5, 3.0, (), jnp.float32)
    cotangent = gaussian(keys[16], (CLIPS, FRAMES, FRAME_TOK, D), 1.0, 6.0, ((0, 8), (1, 4)))
    return dict(patches=patches, mask_ids=mask_ids, action_ids=action_ids, action_table=action_table, action_proj=action_proj, mask_embed=mask_embed, norm_gain=norm_gain, norm_bias=norm_bias, w_qkv=w_qkv, qv_bias=qv_bias, w_out=w_out, out_bias=out_bias, w_fc1=w_fc1, fc1_bias=fc1_bias, w_fc2=w_fc2, fc2_bias=fc2_bias, cotangent=cotangent)


@jax.custom_vjp
def low(v):
    return lax.optimization_barrier(v.astype(jnp.bfloat16)).astype(jnp.float32)

@jax.custom_vjp
def low_back(v):
    return v

def low_keep(v):
    return (low(v), None)

def low_pass(kept, grad):
    return (grad,)

def back_keep(v):
    return (v, None)

def back_low(kept, grad):
    return (low(grad),)
low.defvjp(low_keep, low_pass)
low_back.defvjp(back_keep, back_low)
highest = lax.Precision.HIGHEST
epsilon = 1e-06

def layer_norm(stream, scaling, offset):
    average = lax.optimization_barrier(jnp.mean(stream, axis=-1, keepdims=True))
    centered = stream - average
    variance = lax.optimization_barrier(jnp.mean(centered * centered, axis=-1, keepdims=True))
    return centered * lax.rsqrt(variance + epsilon) * scaling + offset

def to_tubes(hidden):
    frames = hidden.shape[0]
    blocks = GRID // TUBE_W
    shaped = hidden.reshape(frames, blocks, TUBE_W, blocks, TUBE_W, hidden.shape[-1])
    shaped = jnp.transpose(shaped, (1, 3, 0, 2, 4, 5))
    return shaped.reshape(blocks * blocks, frames * TUBE_W * TUBE_W, hidden.shape[-1])

def from_tubes(grouped, frames):
    blocks = GRID // TUBE_W
    shaped = grouped.reshape(blocks, blocks, frames, TUBE_W, TUBE_W, grouped.shape[-1])
    shaped = jnp.transpose(shaped, (2, 0, 3, 1, 4, 5))
    return shaped.reshape(frames, GRID * GRID, grouped.shape[-1])

def attend(queries, key_rows, value_rows):
    groups, length, model_width = queries.shape
    head_size = model_width // HEADS
    query_heads = queries.reshape(groups, length, HEADS, head_size)
    key_heads = key_rows.reshape(groups, length, HEADS, head_size)
    value_heads = value_rows.reshape(groups, length, HEADS, head_size)
    scores = jnp.einsum('glhe,gmhe->ghlm', query_heads, key_heads, precision=highest) * head_size ** (-0.5)
    scores = low_back(scores)
    weights = low(jax.nn.softmax(scores, axis=-1))
    mixed = jnp.einsum('ghlm,gmhe->glhe', weights, value_heads, precision=highest)
    return mixed.reshape(groups, length, model_width)

def block(stream, params, layer, tube):
    norm_gain, norm_bias, w_qkv, qv_bias, w_out, out_bias, w_fc1, fc1_bias, w_fc2, fc2_bias = params
    frames = stream.shape[0]
    model_width = stream.shape[-1]
    hidden = layer_norm(stream, norm_gain[layer, 0], norm_bias[layer, 0])
    if tube:
        grouped = to_tubes(low(low_back(hidden)))
    else:
        grouped = low(hidden)
    projected = jnp.einsum('gld,de->gle', grouped, w_qkv[layer], precision=highest)
    queries = low(low_back(projected[..., :model_width] + qv_bias[layer, 0]))
    key_rows = low(low_back(projected[..., model_width:2 * model_width]))
    value_rows = low(low_back(projected[..., 2 * model_width:] + qv_bias[layer, 1]))
    attended = low(low_back(attend(queries, key_rows, value_rows)))
    if tube:
        attended = from_tubes(attended, frames)
    branch = jnp.einsum('fsd,de->fse', attended, w_out[layer], precision=highest) + out_bias[layer]
    middle = stream + low_back(branch)
    hidden_two = low(layer_norm(middle, norm_gain[layer, 1], norm_bias[layer, 1]))
    before = low_back(jnp.einsum('fsd,dk->fsk', hidden_two, w_fc1[layer], precision=highest) + fc1_bias[layer])
    activated = low(jax.nn.gelu(before))
    mlp_out = jnp.einsum('fsk,kd->fsd', activated, w_fc2[layer], precision=highest) + fc2_bias[layer]
    return middle + low_back(mlp_out)

def forward(params, patch_clip, mask_clip, action_row):
    action_table, action_proj, mask_embed = (params[0], params[1], params[2])
    layer_params = params[3:]
    chosen = action_table[action_row]
    drive = jnp.dot(chosen, action_proj, precision=highest)
    stream = jnp.where(mask_clip[..., None] == 1, mask_embed, patch_clip) + drive[:, None, :]
    stream = block(stream, layer_params, 0, False)
    return block(stream, layer_params, 1, True)

def reference(patches, mask_ids, action_ids, action_table, action_proj, mask_embed, norm_gain, norm_bias, w_qkv, qv_bias, w_out, out_bias, w_fc1, fc1_bias, w_fc2, fc2_bias, cotangent):
    params = tuple((weight.astype(jnp.float32) for weight in (action_table, action_proj, mask_embed, norm_gain, norm_bias, w_qkv, qv_bias, w_out, out_bias, w_fc1, fc1_bias, w_fc2, fc2_bias)))
    initial = jax.tree.map(jnp.zeros_like, params)

    def one_clip(totals, inputs):
        patch_clip, mask_clip, action_row, cotangent_clip = inputs

        def clip_forward(weights, patch_in):
            return forward(weights, patch_in, mask_clip, action_row)
        result, pullback = jax.vjp(clip_forward, params, patch_clip.astype(jnp.float32))
        gradients, patch_grad = pullback(cotangent_clip.astype(jnp.float32))
        totals = jax.tree.map(jnp.add, totals, gradients)
        return (totals, (result.astype(jnp.bfloat16), patch_grad.astype(jnp.bfloat16)))
    totals, outcome = lax.scan(one_clip, initial, (patches, mask_ids, action_ids, cotangent))
    return (outcome[0], outcome[1], totals[0], totals[1], totals[2], totals[3], totals[4], totals[5], totals[6], totals[7], totals[8], totals[9], totals[10], totals[11], totals[12])
```

```python
import functools

import jax
import jax.numpy as jnp
from jax import lax
from jax.experimental import pallas as pl
from jax.experimental.pallas import tpu as pltpu
from jax.sharding import PartitionSpec as P

HEADS = 12
GRID = 16
TUBE_W = 4
TUBES = 16
HEAD = 64
STEP = 256

epsilon = 1e-06
highest = lax.Precision.HIGHEST
f32 = jnp.float32
bf16 = jnp.bfloat16
PARAMS = pltpu.CompilerParams(vmem_limit_bytes=60 * 1024 * 1024)


def wide(value):
    return value.astype(f32)


def narrow(value):
    return value.astype(bf16)


def dot(a, b, a_dim=1, b_dim=0):
    return lax.dot_general(a, b, (((a_dim,), (b_dim,)), ((), ())), preferred_element_type=f32)


def normalize(stream):
    centered = stream - jnp.mean(stream, axis=-1, keepdims=True)
    scale = lax.rsqrt(jnp.mean(centered * centered, axis=-1, keepdims=True) + epsilon)
    return centered * scale, scale


def normalize_back(grad, stream, gain):
    unit, scale = normalize(stream)
    inner = grad * gain
    part = scale * (
        inner
        - jnp.mean(inner, axis=-1, keepdims=True)
        - unit * jnp.mean(inner * unit, axis=-1, keepdims=True)
    )
    return part, rows_sum(grad * unit), rows_sum(grad)


def rows_sum(value):
    return jnp.sum(value, axis=0, keepdims=True)


def gelu_pair(u):
    root = 0.7978845608028654
    square = u * u
    t = jnp.tanh(root * u * (1.0 + 0.044715 * square))
    half = 0.5 * (1.0 + t)
    slope = half + 0.5 * u * (1.0 - t * t) * (root * (1.0 + 3 * 0.044715 * square))
    return u * half, slope


def softmax(scores, group):
    length = scores.shape[0]
    if group < length:
        same = (
            lax.broadcasted_iota(jnp.int32, scores.shape, 0) // group
            == lax.broadcasted_iota(jnp.int32, scores.shape, 1) // group
        )
        scores = jnp.where(same, scores, -1e30)
    expsum = jnp.exp(scores - jnp.max(scores, axis=-1, keepdims=True))
    return expsum / jnp.sum(expsum, axis=-1, keepdims=True)


def low_lanes(length):
    return lax.broadcasted_iota(jnp.int32, (length, 2 * HEAD), 1) < HEAD


def attend_kernel(*refs, first, group, tokens_frame):
    if first:
        (patches, mask, embed, drive, gain, bias, wq, wk, wv, qb, vb) = refs[:11]
        (stream, hidden, q_out, k_out, v_out, mixed) = refs[11:]

        @pl.when(pl.program_id(0) == 0)
        def _():
            for part in range(patches.shape[0] // tokens_frame):
                rows = pl.ds(part * tokens_frame, tokens_frame)
                value = jnp.where(mask[rows, :] == 1, embed[...], wide(patches[rows, :]))
                value = value + drive[pl.ds(part, 1), :]
                stream[rows, :] = value
                hidden[rows, :] = narrow(normalize(value)[0] * gain[0] + bias[0])

    else:
        hidden, wq, wk, wv, qb, vb, q_out, k_out, v_out, mixed = refs
    source = hidden[...]
    q_out[...] = narrow(dot(source, wq[0]) + qb[0])
    k_out[...] = narrow(dot(source, wk[0]))
    v_out[...] = narrow(dot(source, wv[0]) + vb[0])
    length = max(group, 128)
    lanes = low_lanes(length)
    for block in range(source.shape[0] // length):
        rows = pl.ds(block * length, length)
        for pair in range(STEP // (2 * HEAD)):
            columns = pl.ds(pair * 2 * HEAD, 2 * HEAD)
            q, k, v = q_out[rows, columns], k_out[rows, columns], v_out[rows, columns]
            results = []
            for mine in (lanes, ~lanes):
                scores = dot(jnp.where(mine, q, 0), k, 1, 1) * HEAD**-0.5
                results.append(dot(narrow(softmax(scores, group)), v))
            mixed[rows, columns] = narrow(jnp.where(lanes, results[0], results[1]))


def attend_back_kernel(*refs, first, group, tokens_frame):
    if first:
        (go, q_in, k_in, v_in, wq, wk, wv, gain, stream, gmid, mask) = refs[:11]
        (dq_out, dk_out, dv_out, shifts, patch_grad, small, total) = refs[11:]
    else:
        go, q_in, k_in, v_in, wq, wk, wv = refs[:7]
        dq_out, dk_out, dv_out, shifts, grouped, total = refs[7:]
    length = max(group, 128)
    lanes = low_lanes(length)
    for block in range(go.shape[0] // length):
        rows = pl.ds(block * length, length)
        for pair in range(STEP // (2 * HEAD)):
            columns = pl.ds(pair * 2 * HEAD, 2 * HEAD)
            q, k, v = q_in[rows, columns], k_in[rows, columns], v_in[rows, columns]
            g = go[rows, columns]
            results = []
            for mine in (lanes, ~lanes):
                scores = dot(jnp.where(mine, q, 0), k, 1, 1) * HEAD**-0.5
                probs = softmax(scores, group)
                grad = dot(jnp.where(mine, g, 0), v, 1, 1)
                inner = jnp.sum(probs * grad, axis=-1, keepdims=True)
                ds = narrow(probs * (grad - inner))
                results.append(
                    (
                        dot(ds, k) * HEAD**-0.5,
                        dot(ds, q, 0, 0) * HEAD**-0.5,
                        dot(narrow(probs), g, 0, 0),
                    )
                )
            for out, low, high in zip((dq_out, dk_out, dv_out), *results):
                out[rows, columns] = narrow(jnp.where(lanes, low, high))
    dq, dk, dv = dq_out[...], dk_out[...], dv_out[...]
    shifts[...] = jnp.zeros_like(shifts)
    shifts[0:1, :] = rows_sum(wide(dq))
    shifts[1:2, :] = rows_sum(wide(dv))
    part = dot(dq, wq[0], 1, 1) + dot(dk, wk[0], 1, 1) + dot(dv, wv[0], 1, 1)
    step = pl.program_id(0)

    @pl.when(step == 0)
    def _():
        total[...] = part

    @pl.when(step > 0)
    def _():
        total[...] += part

    @pl.when(step == pl.num_programs(0) - 1)
    def _():
        if not first:
            grouped[...] = narrow(total[...])
        else:
            back, gain_grad, bias_grad = normalize_back(total[...], stream[...], gain[0])
            zero = gmid[...] + back
            masked = mask[...] == 1
            patch_grad[...] = narrow(jnp.where(masked, 0.0, zero))
            small[...] = jnp.zeros_like(small)
            small[0:1, :] = gain_grad
            small[1:2, :] = bias_grad
            small[2:3, :] = rows_sum(jnp.where(masked, zero, 0.0))
            for frame in range(zero.shape[0] // tokens_frame):
                small[3 + frame : 4 + frame, :] = rows_sum(
                    zero[frame * tokens_frame : (frame + 1) * tokens_frame]
                )


def mlp_kernel(
    stream, mixed, w_out, out_bias, gain, bias, w_fc1, fc1_bias, w_fc2, fc2_bias, gain_next, bias_next,
    middle, hidden_two, before_out, activated_out, result, hidden,
):
    step = pl.program_id(0)

    @pl.when(step == 0)
    def _():
        value = stream[...] + dot(mixed[...], w_out[0]) + out_bias[0]
        middle[...] = value
        hidden_two[...] = narrow(normalize(value)[0] * gain[0] + bias[0])
        result[...] = value + fc2_bias[0]

    before = dot(hidden_two[...], w_fc1[0]) + fc1_bias[0]
    before_out[...] = before
    activated = narrow(gelu_pair(before)[0])
    activated_out[...] = activated
    result[...] += dot(activated, w_fc2[0])

    @pl.when(step == pl.num_programs(0) - 1)
    def _():
        hidden[...] = narrow(normalize(result[...])[0] * gain_next[0] + bias_next[0])


def mlp_tail(grad, gh2, middle, gain, w_out, gmid, gb_out, go, small):
    back, gain_grad, bias_grad = normalize_back(gh2, middle, gain)
    value = grad + back
    gmid[...] = value
    gb = narrow(value)
    gb_out[...] = gb
    go[...] = narrow(dot(gb, w_out, 1, 1))
    small[0:1, :] = gain_grad
    small[1:2, :] = bias_grad
    small[2:3, :] = rows_sum(wide(gb))


def mlp_both_kernel(
    stream, mixed, w_out, out_bias, gain, bias, w_fc1, fc1_bias, w_fc2, fc2_bias, cotangent,
    output, hidden_two, activated_out, gu_out, gmid, gb, go, small,
    middle, result, gh2,
):
    step = pl.program_id(0)

    @pl.when(step == 0)
    def _():
        value = stream[...] + dot(mixed[...], w_out[0]) + out_bias[0]
        middle[...] = value
        hidden_two[...] = narrow(normalize(value)[0] * gain[0] + bias[0])
        result[...] = value + fc2_bias[0]
        gh2[...] = jnp.zeros_like(gh2)
        small[3:4, :] = rows_sum(wide(cotangent[...]))

    before = dot(hidden_two[...], w_fc1[0]) + fc1_bias[0]
    value, slope = gelu_pair(before)
    activated = narrow(value)
    activated_out[...] = activated
    result[...] += dot(activated, w_fc2[0])
    gu = narrow(slope * dot(cotangent[...], w_fc2[0], 1, 1))
    gu_out[...] = gu
    small[pl.ds(4 + step, 1), :] = rows_sum(wide(gu))
    gh2[...] += dot(gu, w_fc1[0], 1, 1)

    @pl.when(step == pl.num_programs(0) - 1)
    def _():
        output[...] = narrow(result[...])
        mlp_tail(wide(cotangent[...]), gh2[...], middle[...], gain[0], w_out[0], gmid, gb, go, small)


def mlp_back_kernel(
    gmid_next, grad_hidden, stream_next, gain_next, middle, gain, before, w_fc1, w_fc2, w_out,
    gm, gu_out, gmid, gb, go, small, small_next,
    grad, gh2,
):
    step = pl.program_id(0)

    @pl.when(step == 0)
    def _():
        back, gain_grad, bias_grad = normalize_back(
            wide(grad_hidden[...]), stream_next[...], gain_next[0]
        )
        value = gmid_next[...] + back
        grad[...] = value
        low = narrow(value)
        gm[...] = low
        gh2[...] = jnp.zeros_like(gh2)
        small[3:4, :] = rows_sum(wide(low))
        small_next[...] = jnp.zeros_like(small_next)
        small_next[0:1, :] = gain_grad
        small_next[1:2, :] = bias_grad

    gu = narrow(gelu_pair(before[...])[1] * dot(gm[...], w_fc2[0], 1, 1))
    gu_out[...] = gu
    small[pl.ds(4 + step, 1), :] = rows_sum(wide(gu))
    gh2[...] += dot(gu, w_fc1[0], 1, 1)

    @pl.when(step == pl.num_programs(0) - 1)
    def _():
        mlp_tail(grad[...], gh2[...], middle[...], gain[0], w_out[0], gmid, gb, go, small)


def whole_spec(shape):
    return pl.BlockSpec(tuple(shape), lambda *_: (0,) * len(shape))


def vector_spec(row, width):
    return pl.BlockSpec((1, 1, width), lambda *_: (row, 0, 0))


def call(body, grid, inputs, outputs, scratch=(), flops=0):
    moved = sum(a.size * a.dtype.itemsize for a, _ in inputs) // 2
    return pl.pallas_call(
        body,
        grid=grid,
        in_specs=[s or whole_spec(a.shape) for a, s in inputs],
        out_specs=[s or whole_spec(shape) for shape, _, s in outputs],
        out_shape=[jax.ShapeDtypeStruct(shape, dtype) for shape, dtype, _ in outputs],
        scratch_shapes=list(scratch),
        compiler_params=PARAMS,
        cost_estimate=pl.CostEstimate(flops=flops, bytes_accessed=moved, transcendentals=0),
    )(*[a for a, _ in inputs])


def head_specs(w_qkv, layer):
    width = w_qkv.shape[1]
    steps = width // STEP
    return [
        (w_qkv, pl.BlockSpec((1, width, STEP), lambda i, part=part: (layer, 0, i + steps * part)))
        for part in range(3)
    ]


def column_spec(tokens):
    return pl.BlockSpec((tokens, STEP), lambda i: (0, i))


def project_attend(w_qkv, qv_bias, layer, group, start=None, hidden=None, tokens_frame=None):
    first = hidden is None
    tokens, width = (start[0] if first else hidden).shape
    inputs = [(a, None) for a in start[:4]] if first else [(hidden, None)]
    if first:
        inputs += start[4]
    inputs += head_specs(w_qkv, layer)
    flat = qv_bias.reshape(-1, 1, width)
    inputs += [
        (flat, pl.BlockSpec((1, 1, STEP), lambda i, row=2 * layer + part: (row, 0, i))) for part in range(2)
    ]
    outputs = [((tokens, width), bf16, column_spec(tokens))] * 4
    if first:
        outputs = [((tokens, width), f32, None), ((tokens, width), bf16, None)] + outputs
    body = functools.partial(attend_kernel, first=first, group=group, tokens_frame=tokens_frame)
    return call(body, (width // STEP,), inputs, outputs, flops=8 * tokens * width * width)


def project_back(go, queries, key_rows, value_rows, w_qkv, layer, group, extra=None, tokens_frame=None):
    first = extra is not None
    tokens, width = go.shape
    inputs = [(a, column_spec(tokens)) for a in (go, queries, key_rows, value_rows)]
    inputs += head_specs(w_qkv, layer)
    outputs = [((tokens, width), bf16, column_spec(tokens))] * 3
    outputs.append(((8, width), f32, pl.BlockSpec((8, STEP), lambda i: (0, i))))
    if first:
        inputs += extra
        outputs += [((tokens, width), bf16, None), ((8, width), f32, None)]
    else:
        outputs.append(((tokens, width), bf16, None))
    body = functools.partial(attend_back_kernel, first=first, group=group, tokens_frame=tokens_frame)
    return call(
        body,
        (width // STEP,),
        inputs,
        outputs,
        [pltpu.VMEM((tokens, width), f32)],
        flops=10 * tokens * width * width,
    )


def xor_permute(value, axis, flip):
    count = lax.axis_size(axis)
    return lax.ppermute(value, axis, [(i, i ^ flip) for i in range(count)])


def split_columns(arrays, count):
    width = sum(a.shape[1] for a in arrays) // count
    edges = []
    start = 0
    for a in arrays:
        edges.append((start, start + a.shape[1], a))
        start += a.shape[1]
    for block in range(count):
        low, high = block * width, (block + 1) * width
        at = 0
        for begin, end, a in edges:
            lo, hi = max(low, begin), min(high, end)
            if lo < hi:
                yield block, at, hi - lo, a, lo - begin
                at += hi - lo


def side_by_side(product, blocks, pieces):
    rows, columns = product.shape
    if pieces == 1:
        return product.reshape(blocks, rows // blocks, columns)
    cut = product.reshape(blocks, pieces, rows // blocks // pieces, columns)
    return jnp.concatenate([cut[:, i] for i in range(pieces)], axis=-1)


def store_blocks(product, unit, send, keep):
    @pl.when(pl.program_id(0) == 0)
    def _():
        send[unit, 0] = product

    @pl.when(pl.program_id(0) == 1)
    def _():
        keep[unit, 0] = product


def mlp_grad_kernel(order, hidden_two, gu, activated, gm, send, keep, held, *, blocks, count):
    rest = pl.num_programs(1)
    place = order[pl.program_id(0) * rest + pl.program_id(1)]

    @pl.when((pl.program_id(0) == 0) & (pl.program_id(1) == 0))
    def _():
        for block, at, size, a, low in split_columns((gm,), count):
            held[block, :, at : at + size] = a[:, low : low + size]

    store_blocks(narrow(side_by_side(dot(hidden_two[...], gu[...], 0, 0), blocks, 1)), 0, send, keep)
    pieces = activated.shape[1] // hidden_two.shape[1]
    store_blocks(
        narrow(side_by_side(dot(activated[...], held[place], 0, 0), blocks, pieces)), 1, send, keep
    )


def attend_grad_kernel(order, hidden, dq, dk, dv, mixed, gb, send, keep, held, held_out, *, blocks, count):
    rest = pl.num_programs(1)
    place = order[pl.program_id(0) * rest + pl.program_id(1)]

    @pl.when((pl.program_id(0) == 0) & (pl.program_id(1) == 0))
    def _():
        for block, at, size, a, low in split_columns((dq, dk, dv), count):
            held[block, :, at : at + size] = a[:, low : low + size]
        for block, at, size, a, low in split_columns((gb,), count):
            held_out[block, :, at : at + size] = a[:, low : low + size]

    one = side_by_side(dot(hidden[...], held[place], 0, 0), blocks, 1)
    two = side_by_side(dot(mixed[...], held_out[place], 0, 0), blocks, 1)
    store_blocks(narrow(jnp.concatenate((one, two), axis=-1)), 0, send, keep)


def gradient_blocks(mlp, *arrays):
    frame_size, clip_size = lax.axis_size("frame"), lax.axis_size("clip")
    rest = frame_size // 2
    frame = lax.axis_index("frame")
    core, upper = frame % 2, frame // 2
    order = jnp.stack([(upper ^ j) * 2 + (core ^ (1 - r)) for r in range(2) for j in range(rest)])
    tokens, width = arrays[0].shape
    units = 2 if mlp else 1
    shape = (units, rest, clip_size, width // clip_size, 4 * width // frame_size)
    block = (units, 1) + shape[2:]
    in_specs = [pl.BlockSpec(a.shape, lambda r, j, o: (0, 0)) for a in arrays]
    if mlp:
        gu_width = arrays[1].shape[1] // frame_size
        if gu_width % 128 == 0:
            in_specs[1] = pl.BlockSpec((tokens, gu_width), lambda r, j, o: (0, o[r * rest + j]))
        else:
            arrays = list(arrays)
            arrays[1] = jnp.transpose(arrays[1].reshape(tokens, frame_size, gu_width), (1, 0, 2))
            in_specs[1] = pl.BlockSpec(
                (pl.Squeezed(), tokens, gu_width), lambda r, j, o: (o[r * rest + j], 0, 0)
            )
        body = mlp_grad_kernel
        scratch = [pltpu.VMEM((frame_size, tokens, width // frame_size), bf16)]
    else:
        body = attend_grad_kernel
        scratch = [
            pltpu.VMEM((frame_size, tokens, 3 * width // frame_size), bf16),
            pltpu.VMEM((frame_size, tokens, width // frame_size), bf16),
        ]
    out = jax.ShapeDtypeStruct(shape, bf16)
    return pl.pallas_call(
        functools.partial(body, blocks=clip_size, count=frame_size),
        grid_spec=pltpu.PrefetchScalarGridSpec(
            num_scalar_prefetch=1,
            grid=(2, rest),
            in_specs=in_specs,
            out_specs=[
                pl.BlockSpec(block, lambda r, j, o: (0, jnp.where(r == 0, j, rest - 1), 0, 0, 0)),
                pl.BlockSpec(block, lambda r, j, o: (0, jnp.where(r == 0, 0, j), 0, 0, 0)),
            ],
            scratch_shapes=scratch,
        ),
        out_shape=[out, out],
        compiler_params=PARAMS,
        cost_estimate=pl.CostEstimate(
            flops=8 * units * tokens * width * width, bytes_accessed=2**24, transcendentals=0
        ),
    )(order.astype(jnp.int32), *arrays)


def pick(value, index, axis):
    return lax.dynamic_index_in_dim(value, index, axis, keepdims=False)


def reduce_blocks(send, keep):
    clip = lax.axis_index("clip")
    across, along = clip % 2, clip // 2
    along_size = lax.axis_size("clip") // 2
    units, rest, blocks, high, width = keep.shape
    total = narrow(wide(keep) + wide(xor_permute(send, "frame", 1)))
    total = total.reshape(units, rest, along_size, 2, high, width)
    if units == 2:
        one, two = total[0], total[1]
    else:
        one, two = total[0, ..., : high // 2, :], total[0, ..., high // 2 :, :]

    def over_rest(value):
        result = wide(value[0])
        for j in range(1, rest):
            result = result + wide(xor_permute(value[j], "frame", 2 * j))
        return narrow(result)

    def over_across(value, axis):
        arrived = xor_permute(pick(value, 1 - across, axis), "clip", 1)
        return narrow(wide(pick(value, across, axis)) + wide(arrived))

    one = over_across(over_rest(one), 1)
    two = over_rest(over_across(two, 2))
    total = jnp.stack((one, two))
    result = wide(pick(total, along, 1))
    for j in range(1, along_size):
        result = result + wide(xor_permute(pick(total, along ^ j, 1), "clip", 2 * j))
    return result


def flips():
    frame_flips = [("frame", 1 << b) for b in range(lax.axis_size("frame").bit_length() - 1)]
    clip_flips = [("clip", 1 << b) for b in range(lax.axis_size("clip").bit_length() - 1)]
    return frame_flips + clip_flips


def sum_everywhere(*parts):
    flat = jnp.concatenate(parts, axis=0)
    for axis, flip in flips():
        flat = flat + xor_permute(flat, axis, flip)
    return flat


def gather_everywhere(rows):
    for axis, flip in flips():
        rows = jnp.concatenate((rows, xor_permute(rows, axis, flip)), axis=0)
    return rows


def tube_order(value):
    blocks = GRID // TUBE_W
    shaped = value.reshape(value.shape[:2] + (blocks, TUBE_W, blocks, TUBE_W) + value.shape[3:])
    return jnp.swapaxes(shaped, 3, 4).reshape(value.shape)


def frame_order(value):
    blocks = GRID // TUBE_W
    shaped = value.reshape(value.shape[:2] + (blocks, blocks, TUBE_W, TUBE_W) + value.shape[3:])
    return jnp.swapaxes(shaped, 3, 4).reshape(value.shape)


def to_tubes(value, clips):
    shaped = value.reshape(clips, TUBES, 1, TUBE_W * TUBE_W, value.shape[-1])
    arrived = lax.all_to_all(shaped, "frame", split_axis=1, concat_axis=2, tiled=True)
    return arrived.reshape(value.shape)


def to_frames(value, clips):
    size = lax.axis_size("frame")
    shaped = value.reshape(clips, TUBES // size, size, TUBE_W * TUBE_W, value.shape[-1])
    returned = lax.all_to_all(shaped, "frame", split_axis=2, concat_axis=1, tiled=True)
    return returned.reshape(value.shape)


def local(
    patches,
    mask_ids,
    action_ids,
    action_table,
    action_proj,
    mask_embed,
    norm_gain,
    norm_bias,
    w_qkv,
    qv_bias,
    w_out,
    out_bias,
    w_fc1,
    fc1_bias,
    w_fc2,
    fc2_bias,
    cotangent,
):
    actions, width = action_table.shape
    clips, frames, tokens_frame, _ = patches.shape
    tokens = clips * frames * tokens_frame
    hidden_width = w_fc1.shape[2]
    frame_size, clip_size = lax.axis_size("frame"), lax.axis_size("clip")
    tube_group = frame_size * frames * TUBE_W * TUBE_W
    onehot = narrow(action_ids.reshape(-1, 1) == jnp.arange(actions, dtype=jnp.int32))
    chosen = dot(onehot, action_table)
    drive = dot(narrow(chosen), action_proj)
    patches = tube_order(patches).reshape(tokens, width)
    mask = tube_order(mask_ids).reshape(tokens, 1)
    cotangent = tube_order(cotangent).reshape(tokens, width)

    gains = norm_gain.reshape(-1, 1, width)
    biases = norm_bias.reshape(-1, 1, width)
    out_biases = out_bias.reshape(-1, 1, width)
    fc2_biases = fc2_bias.reshape(-1, 1, width)
    fc1_biases = fc1_bias.reshape(-1, 1, hidden_width)

    def norm(layer, place):
        spec = vector_spec(2 * layer + place, width)
        return [(gains, spec), (biases, spec)]

    def layer_weights(layer):
        fc1 = (w_fc1, pl.BlockSpec((1, width, width), lambda i: (layer, 0, i)))
        fc1_shift = (fc1_biases, pl.BlockSpec((1, 1, width), lambda i: (layer, 0, i)))
        fc2 = (w_fc2, pl.BlockSpec((1, width, width), lambda i: (layer, i, 0)))
        out = (w_out, pl.BlockSpec((1, width, width), lambda i: (layer, 0, 0)))
        return fc1, fc1_shift, fc2, out

    chunk = pl.BlockSpec((tokens, width), lambda i: (0, i))
    steps = hidden_width // width
    plain_low = ((tokens, width), bf16, None)
    plain = ((tokens, width), f32, None)
    wide_low = ((tokens, hidden_width), bf16, chunk)
    small_out = ((8, width), f32, None)
    matrix = tokens * width * hidden_width
    held = pltpu.VMEM((tokens, width), f32)

    stream_zero, hidden_zero, q_zero, k_zero, v_zero, mixed_zero = project_attend(
        w_qkv,
        qv_bias,
        0,
        tokens_frame,
        start=(patches, mask, mask_embed.reshape(1, width), drive, norm(0, 0)),
        tokens_frame=tokens_frame,
    )
    fc1, fc1_shift, fc2, out = layer_weights(0)
    middle_zero, hidden_two_zero, before_zero, activated_zero, stream_one, hidden_one = call(
        mlp_kernel,
        (steps,),
        [(stream_zero, None), (mixed_zero, None), out, (out_biases, vector_spec(0, width))]
        + norm(0, 1)
        + [fc1, fc1_shift, fc2, (fc2_biases, vector_spec(0, width))]
        + norm(1, 0),
        [plain, plain_low, ((tokens, hidden_width), f32, chunk), wide_low, plain, plain_low],
        flops=5 * matrix,
    )

    tubes_one = to_tubes(hidden_one, clips)
    q_one, k_one, v_one, mixed_tubes = project_attend(w_qkv, qv_bias, 1, tube_group, hidden=tubes_one)
    mixed_one = to_frames(mixed_tubes, clips)
    fc1, fc1_shift, fc2, out = layer_weights(1)
    output, hidden_two_one, activated_one, gu_one, gmid_one, gb_one, go_one, small_one = call(
        mlp_both_kernel,
        (steps,),
        [(stream_one, None), (mixed_one, None), out, (out_biases, vector_spec(1, width))]
        + norm(1, 1)
        + [fc1, fc1_shift, fc2, (fc2_biases, vector_spec(1, width)), (cotangent, None)],
        [plain_low, plain_low, wide_low, wide_low, plain, plain_low, plain_low, small_out],
        [held, held, held],
        flops=10 * matrix,
    )

    mlp_one = reduce_blocks(*gradient_blocks(True, hidden_two_one, gu_one, activated_one, cotangent))
    dq, dk, dv, shifts_one, grouped = project_back(
        to_tubes(go_one, clips), q_one, k_one, v_one, w_qkv, 1, tube_group
    )
    grad_hidden = to_frames(grouped, clips)
    attend_one = reduce_blocks(
        *gradient_blocks(False, tubes_one, dq, dk, dv, mixed_one, gb_one)
    )

    fc1, fc1_shift, fc2, out = layer_weights(0)
    gm_zero, gu_zero, gmid_zero, gb_zero, go_zero, small_zero, small_next = call(
        mlp_back_kernel,
        (steps,),
        [(gmid_one, None), (grad_hidden, None), (stream_one, None), norm(1, 0)[0]]
        + [(middle_zero, None), norm(0, 1)[0], (before_zero, chunk), fc1, fc2, out],
        [plain_low, wide_low, plain, plain_low, plain_low, small_out, small_out],
        [held, held],
        flops=5 * matrix,
    )
    mlp_zero = reduce_blocks(*gradient_blocks(True, hidden_two_zero, gu_zero, activated_zero, gm_zero))
    dq, dk, dv, shifts_zero, patch_grad, small_first = project_back(
        go_zero,
        q_zero,
        k_zero,
        v_zero,
        w_qkv,
        0,
        tokens_frame,
        extra=[norm(0, 0)[0], (stream_zero, None), (gmid_zero, None), (mask, None)],
        tokens_frame=tokens_frame,
    )
    attend_zero = reduce_blocks(*gradient_blocks(False, hidden_zero, dq, dk, dv, mixed_zero, gb_zero))

    gathered = gather_everywhere(
        jnp.concatenate(
            (
                small_first[3 : 3 + clips * frames],
                jnp.broadcast_to(wide(action_ids).reshape(-1, 1), (action_ids.size, 128)),
            ),
            axis=1,
        )
    )
    drive_all = gathered[:, :width]
    ids_all = gathered[:, width].astype(jnp.int32)
    clip, frame = lax.axis_index("clip"), lax.axis_index("frame")
    row_count, column_count = width // clip_size, width // frame_size
    act_count = actions // clip_size
    onehot_all = wide(ids_all[:, None] == jnp.arange(actions, dtype=jnp.int32))
    table_rows = wide(lax.dynamic_slice_in_dim(action_table, clip * row_count, row_count, 1))
    proj_sum = lax.dot_general(
        jnp.dot(onehot_all, table_rows, precision=highest),
        lax.dynamic_slice_in_dim(drive_all, frame * column_count, column_count, 1),
        (((0,), (0,)), ((), ())),
        precision=highest,
    )
    chosen_grad = lax.dot_general(
        drive_all,
        wide(lax.dynamic_slice_in_dim(action_proj, frame * column_count, column_count, 0)),
        (((1,), (1,)), ((), ())),
        precision=highest,
    )
    table_sum = lax.dot_general(
        lax.dynamic_slice_in_dim(onehot_all, clip * act_count, act_count, 1),
        chosen_grad,
        (((0,), (0,)), ((), ())),
        precision=highest,
    )

    def attend_parts(value):
        value = jnp.concatenate((value[0], value[1]), axis=0)
        return value[:, : 3 * column_count], value[:, 3 * column_count :]

    def mlp_parts(value):
        pieces = [value[1][:, i * column_count : (i + 1) * column_count] for i in range(steps)]
        return value[0], jnp.concatenate(pieces, axis=0)

    (qkv_a, out_a), (qkv_b, out_b) = attend_parts(attend_zero), attend_parts(attend_one)
    (fc1_a, fc2_a), (fc1_b, fc2_b) = mlp_parts(mlp_zero), mlp_parts(mlp_one)

    upper = sum_everywhere(small_one, shifts_one)
    lower = sum_everywhere(small_zero, small_next, shifts_zero, small_first)

    def rows(*values):
        return jnp.concatenate([v.reshape(1, -1) for v in values], axis=0)

    norm_shape = (2, 2, width)
    gain_grad = rows(lower[24], lower[0], lower[8], upper[0]).reshape(norm_shape)
    bias_grad = rows(lower[25], lower[1], lower[9], upper[1]).reshape(norm_shape)
    shape = (clips, frames, tokens_frame, width)
    return (
        frame_order(output.reshape(shape)),
        frame_order(patch_grad.reshape(shape)),
        table_sum,
        proj_sum,
        lower[26],
        gain_grad,
        bias_grad,
        jnp.stack((qkv_a, qkv_b)),
        jnp.concatenate((lower[16:18], upper[8:10])).reshape(norm_shape),
        jnp.stack((out_a, out_b)),
        rows(lower[2], upper[2]),
        jnp.stack((fc1_a, fc1_b)),
        rows(lower[4 : 4 + steps], upper[4 : 4 + steps]),
        jnp.stack((fc2_a, fc2_b)),
        rows(lower[3], upper[3]),
    )


def solution(mesh):
    rows = P("clip", "frame", None, None)
    blocks = P(None, "clip", "frame")
    in_specs = (rows, P("clip", "frame", None), P("clip", "frame")) + (P(),) * 13 + (rows,)
    out_specs = (
        rows, rows, P("clip", "frame"), P("clip", "frame"), P(), P(), P(),
        blocks, P(), blocks, P(), blocks, P(), blocks, P(),
    )
    return jax.shard_map(local, mesh=mesh, in_specs=in_specs, out_specs=out_specs, check_vma=False)
```
